32 devices in a mesh: dp: 16 (over z, x, core), tp: 2 (over y).
Axes of the slice: x: 2, y: 2, z: 4, core: 2. Of those that a mesh axis runs over, the one named last changes fastest.
Arguments:
- tokens: bfloat16 [4096, 2560], P('dp', 'tp'), may hold values from -16 to 16, as said below
- master: float32 [3, 14336, 2560], P(None, ('dp', 'tp')), may hold values from -1 to 1, as said below
- gradients: bfloat16 [3, 14336, 2560], P(None, ('dp', 'tp')), may hold values from -12 to 12
- first_moment: float32 [3, 14336, 2560], P(None, ('dp', 'tp')), may hold values from -6 to 6
- second_moment: float32 [3, 14336, 2560], P(None, ('dp', 'tp')), may hold values from 1 to 16
- unit_scales: float32 [2, 14336], P(None, ('dp', 'tp')), may hold values from 0.25 to 1.75
- mix_rate: float32 [2560], replicated, may hold values from 0.1 to 0.6
Outputs:
- decoded: bfloat16 [4096, 2560], P('dp', 'tp')
The draws below stay inside these ranges and needn't reach their ends.
Inputs may be any that keep to these rules, and one draw needn't show every extreme that they name: `tokens`: each token's features have root-mean-square close to one. `master`: each row of each of the three matrices has unit length.
All inputs are finite; a program needn't handle non-finite values.
Results may differ from the reference program's by a relative error of at most 0.0085.
Values may be sent and summed in bfloat16 or wider, within the bound.
A program may use at most 256 MiB of HBM per device.

```python
import math
import jax
import jax.numpy as jnp
from jax import lax

D = 2560
FFW = 14336
TOKENS = 4096


def column_profile(key, spread, width_count):
    ramp_scale = jnp.exp(jnp.log(spread) * (jnp.arange(width_count, dtype=jnp.float32) / (width_count - 1) - 0.5))
    roughness = jax.random.uniform(key, (width_count,), jnp.float32, 0.6, 1.4)
    return ramp_scale * roughness


def draw_tokens(key, part):
    key_base = jax.random.fold_in(key, 11)
    key_profile = jax.random.fold_in(key, 12)
    base_values = jnp.clip(jax.random.normal(key_base, (TOKENS, D), jnp.float32), -5.0, 5.0)
    profile = column_profile(key_profile, 3.0, D)
    values = base_values * profile[None, :]
    values = values / jnp.sqrt(jnp.mean(values * values, axis=1, keepdims=True) + 1e-06)
    return values.astype(jnp.bfloat16)


def draw_master(key, part):
    key_base = jax.random.fold_in(key, 21)
    key_flat = jax.random.fold_in(key, 22)
    key_ramp = jax.random.fold_in(key, 23)
    base_values = jnp.clip(jax.random.normal(key_base, (3, FFW, D), jnp.float32), -5.0, 5.0)
    ramp = column_profile(key_ramp, 3.0, D)
    flat_scale = jax.random.uniform(key_flat, (2, 1, D), jnp.float32, 0.6, 1.4)
    profile = jnp.concatenate([flat_scale, ramp[None, None, :]], axis=0)
    values = base_values * profile
    values = values / jnp.sqrt(jnp.sum(values * values, axis=2, keepdims=True) + 1e-06)
    return values.astype(jnp.float32)


def block_scale(own_key, dims, pieces, smallest, largest):
    level = 1.0
    for dim, parts in pieces:
        heights = jax.random.uniform(jax.random.fold_in(jax.random.fold_in(own_key, 6), dim), (parts,), jnp.float32, smallest / len(pieces), largest / len(pieces))
        level = level * jnp.repeat(jnp.exp(heights), dims[dim] // parts).reshape((-1,) + (1,) * (len(dims) - 1 - dim))
    return level


def noise(stream_key, dims, deviation, most, pieces=(), kind=jnp.bfloat16):
    values = jax.random.normal(stream_key, dims, jnp.float32) * deviation
    if len(pieces) > 0:
        values = block_scale(stream_key, dims, pieces, -0.22, 0.18) * values
    return jnp.clip(values, min=-most, max=most).astype(kind)


def setup_inputs(seed: int = 0) -> dict:
    key_list = jax.random.split(jax.random.key(seed), 8)
    return {
        "tokens": draw_tokens(jax.random.fold_in(key_list[7], 71), 0),
        "master": draw_master(jax.random.fold_in(key_list[7], 71), 0),
        "gradients": noise(key_list[2], (3, FFW, D), 3.0, 12.0, ((1, 32),)),
        "first_moment": noise(key_list[3], (3, FFW, D), 1.0, 6.0, ((1, 32),), jnp.float32),
        "second_moment": jnp.clip(jnp.exp(math.log(16.0) - 2.7725887 * jax.random.uniform(key_list[4], (3, FFW, D), jnp.float32) ** block_scale(key_list[4], (3, FFW, D), ((1, 32),), -0.2, 0.2)), 1.0, 16.0),
        "unit_scales": jnp.clip(1.0 + 0.15 * jax.random.normal(key_list[5], (2, FFW), jnp.float32), 0.25, 1.75),
        "mix_rate": jnp.clip(jax.random.uniform(key_list[6], (D,), jnp.float32, 0.1, 0.6), 0.1, 0.6),
    }


beta_first = 0.9
beta_second = 0.95
learn_rate = 0.02
adam_steps = 20
epsilon = 1e-06

def adam_unit(master, gradients, first_moment, second_moment):
    gradient = gradients.astype(jnp.float32)
    moment_one = beta_first * first_moment + (1.0 - beta_first) * gradient
    moment_two = beta_second * second_moment + (1.0 - beta_second) * gradient * gradient
    stepped = master - learn_rate * (moment_one / (1.0 - beta_first ** adam_steps)) / (jnp.sqrt(moment_two / (1.0 - beta_second ** adam_steps)) + 1e-08)
    lengths = jnp.sqrt(lax.optimization_barrier(jnp.sum(stepped * stepped, axis=-1, keepdims=True)) + epsilon)
    return (stepped / lengths).astype(jnp.bfloat16)

def reference(tokens, master, gradients, first_moment, second_moment, unit_scales, mix_rate):
    unit_rows = adam_unit(master, gradients, first_moment, second_moment)
    scales_bf = lax.optimization_barrier(unit_scales.astype(jnp.bfloat16)).astype(jnp.float32)
    gate_in = jnp.dot(tokens, unit_rows[0].T, preferred_element_type=jnp.float32) * scales_bf[0][None, :]
    up_in = jnp.dot(tokens, unit_rows[1].T, preferred_element_type=jnp.float32) * scales_bf[1][None, :]
    hidden = (jax.nn.silu(gate_in) * up_in).astype(jnp.bfloat16)
    branch = jnp.dot(hidden, unit_rows[2], preferred_element_type=jnp.float32)
    branch_rms = jnp.sqrt(lax.optimization_barrier(jnp.mean(branch * branch, axis=1, keepdims=True)) + epsilon)
    inputs = tokens.astype(jnp.float32)
    mix_rates = mix_rate[None, :]
    mixed_state = inputs + mix_rates * (branch / branch_rms - inputs)
    mixed_rms = jnp.sqrt(lax.optimization_barrier(jnp.mean(mixed_state * mixed_state, axis=1, keepdims=True)) + epsilon)
    return (mixed_state / mixed_rms).astype(jnp.bfloat16)
```

```python
import functools

import jax
import jax.numpy as jnp
from jax import lax
from jax.experimental import pallas as pl
from jax.experimental.pallas import tpu as pltpu
from jax.sharding import PartitionSpec as P

beta_first = 0.9
beta_second = 0.95
learn_rate = 0.02
adam_steps = 20
epsilon = 1e-06


def adam_unit(master, gradients, first_moment, second_moment):
    gradient = gradients.astype(jnp.float32)
    moment_one = beta_first * first_moment + (1.0 - beta_first) * gradient
    moment_two = beta_second * second_moment + (1.0 - beta_second) * gradient * gradient
    stepped = master - learn_rate * (moment_one / (1.0 - beta_first**adam_steps)) / (
        jnp.sqrt(moment_two / (1.0 - beta_second**adam_steps)) + 1e-08
    )
    lengths = jnp.sqrt(jnp.sum(stepped * stepped, axis=-1, keepdims=True) + epsilon)
    return (stepped / lengths).astype(jnp.bfloat16)


def branch_kernel(tokens_ref, own_ref, other_ref, scales_ref, out_ref):
    before, parts, after, count, width = tokens_ref.shape
    hidden = []
    for holder, rows_ref in enumerate((own_ref, other_ref)):
        projected = []
        for index in range(2):
            total = None
            for part in range(parts):
                term = lax.dot_general(
                    tokens_ref[:, part].reshape(before * after * count, width),
                    rows_ref[index, part],
                    (((1,), (1,)), ((), ())),
                    preferred_element_type=jnp.float32,
                )
                total = term if total is None else total + term
            projected.append(total * scales_ref[2 * holder + index : 2 * holder + index + 1, :])
        gate_in, up_in = projected
        hidden.append((gate_in / (1.0 + jnp.exp(-gate_in)) * up_in).astype(jnp.bfloat16))
    for part in range(parts):
        share = jnp.dot(hidden[0], own_ref[2, part], preferred_element_type=jnp.float32)
        share += jnp.dot(hidden[1], other_ref[2, part], preferred_element_type=jnp.float32)
        out_ref[:, part] = share.astype(jnp.bfloat16).reshape(before, after, count, width)


def branch_shares(gathered, own_rows, other_rows, scales):
    before, parts, after, count, width = gathered.shape
    units = own_rows.shape[2]
    block_before, block_after = before, after
    while block_before * block_after * count > 512 and block_before % 2 == 0:
        block_before //= 2
    while block_before * block_after * count > 512 and block_after % 2 == 0:
        block_after //= 2
    block = pl.BlockSpec((block_before, parts, block_after, count, width), lambda i, j: (i, 0, j, 0, 0))
    rows_block = pl.BlockSpec(own_rows.shape, lambda i, j: (0, 0, 0, 0))
    tokens_here = before * after * count
    return pl.pallas_call(
        branch_kernel,
        grid=(before // block_before, after // block_after),
        in_specs=[block, rows_block, rows_block, pl.BlockSpec(scales.shape, lambda i, j: (0, 0))],
        out_specs=block,
        out_shape=jax.ShapeDtypeStruct(gathered.shape, jnp.bfloat16),
        cost_estimate=pl.CostEstimate(
            flops=12 * tokens_here * units * parts * width,
            bytes_accessed=4 * gathered.size + 4 * own_rows.size,
            transcendentals=2 * tokens_here * units,
        ),
        compiler_params=pltpu.CompilerParams(vmem_limit_bytes=56 * 1024 * 1024),
    )(gathered, own_rows, other_rows, scales)


def ring_pairs(axis, sizes, shift):
    if axis == "tp":
        return [(i, (i + shift) % sizes["tp"]) for i in range(sizes["tp"])]
    outer, inner = sizes["outer"], sizes["inner"]
    pairs = []
    for o in range(outer):
        for i in range(inner):
            target = ((o + shift) % outer, i) if axis == "outer" else (o, (i + shift) % inner)
            pairs += [
                ((o * inner + i) * 2 + core, (target[0] * inner + target[1]) * 2 + core) for core in range(2)
            ]
    return pairs


def pass_on(value, axis, sizes, shift):
    return lax.ppermute(value, "tp" if axis == "tp" else "dp", ring_pairs(axis, sizes, shift))


def collect(value, order, sizes):
    for axis in order:
        held = [value]
        for _ in range(sizes[axis] - 1):
            held.append(pass_on(held[-1], axis, sizes, 1))
        value = jnp.stack(held)
    return value


def spread_sums(value, order, sizes):
    for axis in reversed(order):
        last = sizes[axis] - 1
        total = value[last]
        for slot in range(last - 1, -1, -1):
            received = pass_on(total, axis, sizes, -1)
            total = (received.astype(jnp.float32) + value[slot].astype(jnp.float32)).astype(jnp.bfloat16)
        value = total
    return value


def shards(dp, tp, tokens, master, gradients, first_moment, second_moment, unit_scales, mix_rate):
    own, share_width = tokens.shape
    model_width = share_width * tp
    outer = 4 if dp % 8 == 0 else 1
    sizes = {"outer": outer, "inner": dp // (2 * outer), "tp": tp}
    third = own // 48 * 16
    cuts = (0, own - 2 * third, own - third, own)
    orders = (("outer", "inner", "tp"), ("inner", "tp", "outer"), ("tp", "outer", "inner"))
    gathered = [
        collect(tokens[cuts[n] : cuts[n + 1]], orders[n], sizes) for n in range(3)
    ]
    unit_rows = adam_unit(master, gradients, first_moment, second_moment)
    scales = unit_scales.astype(jnp.bfloat16)
    swap = [(i, i ^ 1) for i in range(dp)]
    place = lax.axis_index("tp")
    own_rows = jnp.stack(
        [
            lax.dynamic_slice_in_dim(unit_rows, (place + tp - slot) % tp * share_width, share_width, 2)
            for slot in range(tp)
        ],
        axis=1,
    )
    other_rows = lax.ppermute(own_rows, "dp", swap)
    both_scales = jnp.concatenate([scales, lax.ppermute(scales, "dp", swap)]).astype(jnp.float32)
    pieces = []
    for block, order in zip(gathered, orders):
        axes = tuple(reversed(order))
        at = axes.index("tp")
        before = after = 1
        for axis in axes[:at]:
            before *= sizes[axis]
        for axis in axes[at + 1 :]:
            after *= sizes[axis]
        flat = block.reshape((before, tp, after) + block.shape[3:])
        partial = branch_shares(flat, own_rows, other_rows, both_scales)
        pieces.append(spread_sums(partial.reshape(block.shape), order, sizes))
    shares = jnp.concatenate(pieces, axis=0).astype(jnp.float32)
    inputs_local = tokens.astype(jnp.float32)
    column_start = lax.axis_index("tp") * share_width
    mix_rates = lax.dynamic_slice_in_dim(mix_rate, column_start, share_width, 0)[None, :]
    kept_part = (1.0 - mix_rates) * inputs_local
    moved_part = mix_rates * shares
    totals = lax.psum(
        jnp.stack([
            jnp.sum(shares * shares, axis=1),
            jnp.sum(kept_part * kept_part, axis=1),
            jnp.sum(kept_part * moved_part, axis=1),
            jnp.sum(moved_part * moved_part, axis=1),
        ]),
        "tp",
    )
    branch_rms = jnp.sqrt(totals[0] / model_width + epsilon)
    mixed_state = inputs_local + mix_rates * (shares / branch_rms[:, None] - inputs_local)
    mean_square = (
        totals[1] + 2.0 * totals[2] / branch_rms + totals[3] / (branch_rms * branch_rms)
    ) / model_width
    result = mixed_state / jnp.sqrt(mean_square + epsilon)[:, None]
    return result.astype(jnp.bfloat16)


def solution(mesh):
    placed = (
        P("dp", "tp"),
        P(None, ("dp", "tp"), None),
        P(None, ("dp", "tp"), None),
        P(None, ("dp", "tp"), None),
        P(None, ("dp", "tp"), None),
        P(None, ("dp", "tp")),
        P(),
    )
    body = functools.partial(shards, mesh.shape["dp"], mesh.shape["tp"])
    return jax.shard_map(
        body, mesh=mesh, in_specs=placed, out_specs=P("dp", "tp"), check_vma=False
    )
```
